256 devices in a mesh: tx: 16 (over x, y), ty: 16 (over z, core).
Axes of the slice: x: 4, y: 4, z: 8, core: 2. Of those that a mesh axis runs over, the one named last changes fastest.
Arguments:
- members: bfloat16 [128, 64, 512, 128], P('tx', 'ty'), may hold values from -4 to 4
- mean_state: float32 [128, 64, 512], P('tx', 'ty'), may hold values from -6 to 6
- obs_pert: bfloat16 [128, 64, 128, 128], P('tx', 'ty'), may hold values from -1.5 to 1.5
- obs_rinv: bfloat16 [128, 64, 128], P('tx', 'ty'), may hold values from 0.25 to 2
- innovation: bfloat16 [128, 64, 128], P('tx', 'ty'), may hold values from -12 to 12
- obs_count: int32 [128, 64], P('tx', 'ty'), may hold values from 1 to 128, as said below
- neighbours: int32 [128, 64, 12], P('tx', 'ty'), may hold values from 0 to 24, as said below
- loc_weight: float32 [128, 64, 12], P('tx', 'ty'), may hold values from 0.1 to 1
Outputs:
- analysis: bfloat16 [128, 64, 512, 128], P('tx', 'ty')
The draws below stay inside these ranges and needn't reach their ends.
Inputs may be any that keep to these rules, and one draw needn't show every extreme that they name: `obs_count`: counts run from 1 to 128; 128 is reached on some blocks of every device. `neighbours`: the 12 codes of a group are distinct, each naming an offset (c // 5 - 2, c % 5 - 2) of at most two blocks per direction.
All inputs are finite; a program needn't handle non-finite values.
Results may differ from the reference program's by a relative error of at most 0.0049.
Values may be sent and summed in bfloat16 or wider, within the bound.
No kernel may reach another device: no remote copies, remote signals or barrier semaphores. Data moves between devices by JAX's collectives and lax.ppermute only.
A program may use at most 128 MiB of HBM per device.

```python
import math
import jax
import jax.numpy as jnp
from jax import lax

K = 128
OBS_B = 128
NL = 12
NSI = 5
CL = 512
OBX = 128
OBY = 64


def draw_innovation(key, part):
    rows = jnp.arange(OBX, dtype=jnp.float32)[:, None, None] / max(OBX - 1, 1)
    cols = jnp.arange(OBY, dtype=jnp.float32)[None, :, None] / max(OBY - 1, 1)
    scale = 0.6 * (1.0 + rows + cols)
    values = scale * jax.random.normal(jax.random.fold_in(key, 12), (OBX, OBY, OBS_B), jnp.float32)
    return jnp.clip(values, -12.0, 12.0).astype(jnp.bfloat16)


def draw_obs_count(key, part):
    base = jax.random.randint(jax.random.fold_in(key, 21), (OBX, OBY), 1, OBS_B + 1)
    skewed = jnp.maximum(1, base * base // OBS_B)
    flat = jnp.arange(OBX * OBY, dtype=jnp.int32).reshape(OBX, OBY)
    return jnp.where(flat % 7 == 3, OBS_B, skewed).astype(jnp.int32)


def draw_neighbours(key, part):
    scores = jax.random.randint(jax.random.fold_in(key, 31), (OBX, OBY, 25), 0, 2 ** 20) * 32
    scores = scores + jnp.arange(25, dtype=jnp.int32)
    order = jnp.argsort(scores, axis=-1)
    return order[:, :, :NL].astype(jnp.int32)


def block_levels(key, dims, shards, smallest, high):
    factor_of = 1.0
    for axis_at, shards_of in shards:
        heights = jax.random.uniform(jax.random.fold_in(jax.random.fold_in(key, 6), axis_at), (shards_of,), jnp.float32, smallest / len(shards), high / len(shards))
        factor_of = factor_of * jnp.repeat(jnp.exp(heights), dims[axis_at] // shards_of).reshape((-1,) + (1,) * (len(dims) - 1 - axis_at))
    return factor_of


def normal_values(stream_key, shape, spread, reach, shards=(), kind=jnp.bfloat16):
    factor_of = block_levels(stream_key, shape, shards, -0.22, 0.18) if shards else 1.0
    array = jax.random.normal(stream_key, shape, jnp.float32) * spread * factor_of
    return jnp.minimum(jnp.maximum(array, -reach), reach).astype(kind)


def setup_inputs(seed: int = 0) -> dict:
    arg_keys = jax.random.split(jax.random.key(seed), 9)
    return {
        "members": normal_values(arg_keys[0], (OBX, OBY, CL, K), 0.5, 4.0, ((0, 16), (1, 16))),
        "mean_state": normal_values(arg_keys[1], (OBX, OBY, CL), 1.0, 6.0, ((0, 16), (1, 16)), jnp.float32),
        "obs_pert": normal_values(arg_keys[2], (OBX, OBY, OBS_B, K), 0.25, 1.5, ((0, 16), (1, 16))),
        "obs_rinv": jnp.clip(jnp.exp(math.log(2.0) - 2.0794415 * jax.random.uniform(arg_keys[3], (OBX, OBY, OBS_B), jnp.float32) ** block_levels(arg_keys[3], (OBX, OBY, OBS_B), ((0, 16), (1, 16)), -0.2, 0.2)), 0.25, 2.0).astype(jnp.bfloat16),
        "innovation": draw_innovation(jax.random.fold_in(arg_keys[8], 71), 0),
        "obs_count": draw_obs_count(jax.random.fold_in(arg_keys[8], 71), 0),
        "neighbours": draw_neighbours(jax.random.fold_in(arg_keys[8], 71), 0),
        "loc_weight": jnp.clip(0.1 + 0.9 * jax.random.uniform(arg_keys[7], (OBX, OBY, NL), jnp.float32) ** block_levels(arg_keys[7], (OBX, OBY, NL), ((0, 16), (1, 16)), -0.2, 0.2), 0.1, 1.0),
    }


def transform(cmat, vsum, rho):
    width = cmat.shape[-1]
    identity = jnp.eye(width, dtype=jnp.float32)
    matrix = cmat + (width - 1) / rho * identity
    cnorm = jnp.sqrt(lax.optimization_barrier(jnp.sum(matrix * matrix, axis=(1, 2))))[:, None, None]
    root_iter = matrix / cnorm
    inv_iter = jnp.broadcast_to(identity, matrix.shape)
    for sweep in range(NSI):
        update = 1.5 * identity - 0.5 * jnp.einsum('gkl,glm->gkm', inv_iter, root_iter, precision=lax.Precision.HIGHEST)
        root_iter = jnp.einsum('gkl,glm->gkm', root_iter, update, precision=lax.Precision.HIGHEST)
        inv_iter = jnp.einsum('gkl,glm->gkm', update, inv_iter, precision=lax.Precision.HIGHEST)
    covar = jnp.einsum('gkl,glm->gkm', inv_iter, inv_iter, precision=lax.Precision.HIGHEST) / cnorm
    wbar = jnp.einsum('gkl,gl->gk', covar, vsum, precision=lax.Precision.HIGHEST)
    return jnp.sqrt(jnp.float32(width - 1)) * inv_iter / jnp.sqrt(cnorm) + wbar[:, :, None]

def reference(members, mean_state, obs_pert, obs_rinv, innovation, obs_count, neighbours, loc_weight):
    width = obs_pert.shape[3]
    slots = jnp.arange(obs_pert.shape[2], dtype=jnp.int32)
    live_slot = slots[None, None, :] < obs_count[:, :, None]
    obs_weight = jnp.where(live_slot, obs_rinv.astype(jnp.float32), jnp.float32(0.0))
    innov_f = innovation.astype(jnp.float32)
    pert_f = obs_pert.astype(jnp.float32)
    first_sum = jnp.sum(obs_weight * innov_f * innov_f)
    second_sum = jnp.sum(live_slot.astype(jnp.float32) + obs_weight * lax.optimization_barrier(jnp.sum(pert_f * pert_f, axis=-1)) / (width - 1))
    rho = first_sum / second_sum
    scaled = (pert_f * obs_weight[..., None]).astype(jnp.bfloat16).astype(jnp.float32)
    grams = jnp.einsum('abok,abol->abkl', scaled, pert_f, precision=lax.Precision.HIGHEST)
    vectors = jnp.einsum('abok,abo->abk', scaled, innov_f, precision=lax.Precision.HIGHEST)
    column_ids = jnp.arange(OBY, dtype=jnp.int32)

    def group_row(row):
        codes = neighbours[row]
        row_ids = jnp.mod(row + codes // 5 - 2, OBX).astype(jnp.int32)
        col_ids = jnp.mod(column_ids[:, None] + codes % 5 - 2, OBY).astype(jnp.int32)
        picked = grams[row_ids, col_ids]
        picked_v = vectors[row_ids, col_ids]
        cmat = jnp.einsum('jn,jnkl->jkl', loc_weight[row], picked, precision=lax.Precision.HIGHEST)
        vsum = jnp.einsum('jn,jnk->jk', loc_weight[row], picked_v, precision=lax.Precision.HIGHEST)
        return transform(cmat, vsum, rho)
    weights = lax.map(group_row, jnp.arange(OBX, dtype=jnp.int32))

    def analyse_row(row):
        centre = weights[row]
        upper = weights[jnp.mod(row + 1, OBX)]
        lower = weights[jnp.mod(row - 1, OBX)]
        blended = (4.0 * centre + upper + lower + jnp.roll(centre, -1, axis=0) + jnp.roll(centre, 1, axis=0)) / 8.0
        blended = blended.astype(jnp.bfloat16).astype(jnp.float32)
        result = jnp.einsum('brk,bkm->brm', members[row].astype(jnp.float32), blended, precision=lax.Precision.HIGHEST)
        return (result + mean_state[row][:, :, None]).astype(jnp.bfloat16)
    return lax.map(analyse_row, jnp.arange(OBX, dtype=jnp.int32))
```

```python
import jax
import jax.numpy as jnp
from jax import lax
from jax.experimental import pallas as pl
from jax.experimental.pallas import tpu as pltpu
from jax.sharding import Mesh
from jax.sharding import PartitionSpec as P

F32 = jnp.float32
BF16 = jnp.bfloat16
NSI = 5
WIDE = 3
ROWS = 144
BATCH_ROWS = 2
AXES = ("x", "y", "z", "c")
TX = ("x", "y")
TY = ("z", "c")


def ring(count, shift):
    return [(i, (i + shift) % count) for i in range(count)]


def split(value):
    high = value.astype(BF16)
    return high, (value - high.astype(F32)).astype(BF16)


def product(left, right):
    lhs = jnp.concatenate(left, axis=1)
    top = jnp.concatenate(right, axis=1)
    rhs = jnp.concatenate([top, top], axis=0)
    both = jnp.dot(lhs, rhs, preferred_element_type=F32)
    half = both.shape[1] // 2
    return both[:, :half] + both[:, half:]


def block_terms(block, gram_ref, vec_ref, slot):
    pert = block[:128]
    extra = block[128:].astype(F32)
    weight, innov = extra[0:1], extra[1:2]
    scaled = (pert.astype(F32).T * weight).astype(BF16)
    high, low = split(weight * innov)
    line = lax.broadcasted_iota(jnp.int32, (16, 128), 0)
    tail = jnp.where(
        line == 0,
        jnp.broadcast_to(high.astype(F32), (16, 128)),
        jnp.where(line == 1, jnp.broadcast_to(low.astype(F32), (16, 128)), 0.0),
    ).astype(BF16)
    lhs = jnp.concatenate([scaled, tail], axis=0)
    terms = jnp.dot(lhs, pert, preferred_element_type=F32)
    gram_ref[slot] = terms[:128]
    vec_ref[slot] = terms[128:136]


def make_kernel(gx, gy, cl, listed):
    outer_y = gy + 2 * WIDE
    ring_y = gy + 2
    batch = BATCH_ROWS * ring_y
    batches = (gx + 2) // BATCH_ROWS

    def kernel(
        target_ref, factor_ref, shift_ref,
        own_ref, low_ref, high_ref, left_ref, right_ref, cleft_ref, cright_ref,
        mean_ref, members_ref, out_ref,
        gram_ref, vec_ref, weight_ref, root_ref, inv_ref, upd_ref, side_ref, norm_ref,
        held_ref, stage_ref, in_sem, out_sem,
    ):
        fetch = pltpu.make_async_copy(members_ref, held_ref, in_sem)
        fetch.start()

        def piece(ref, row0, col0, rows_split=None):
            nrow, ncol = ref.shape[0], ref.shape[1]

            @pl.loop(0, nrow)
            def _(r):
                if rows_split is None:
                    base = (r + row0) * outer_y
                else:
                    base = (r + jnp.where(r >= rows_split, gx, 0) + row0) * outer_y
                for c in range(ncol):
                    block_terms(ref[r, c], gram_ref, vec_ref, base + (col0 + c))

        piece(own_ref, WIDE, WIDE)
        piece(low_ref, 0, WIDE)
        piece(high_ref, WIDE + gx, WIDE)
        piece(left_ref, WIDE, 0)
        piece(right_ref, WIDE, WIDE + gy)
        piece(cleft_ref, 0, 0, WIDE)
        piece(cright_ref, 0, WIDE + gy, WIDE)

        eye = (
            lax.broadcasted_iota(jnp.int32, (128, 128), 0)
            == lax.broadcasted_iota(jnp.int32, (128, 128), 1)
        )
        shift = shift_ref[0]

        def update_of(value, g):
            upd = jnp.where(eye, 1.5, 0.0) - 0.5 * value
            high, low = split(upd)
            upd_ref[g, 0] = high
            upd_ref[g, 1] = low

        def keep(ref, g, value):
            high, low = split(value)
            ref[g, 0] = high
            ref[g, 1] = low

        def pair(ref, g):
            return ref[g, 0], ref[g, 1]

        @pl.loop(0, batches)
        def _(b):
            for g in range(batch):
                line = b * batch + g
                total = jnp.zeros((128, 128), F32)
                vsum = jnp.zeros((8, 128), F32)
                for j in range(listed):
                    slot = target_ref[line, j]
                    factor = factor_ref[line, j]
                    total = total + factor * gram_ref[slot]
                    vsum = vsum + factor * vec_ref[slot]
                matrix = total + jnp.where(eye, shift, 0.0)
                norm = jnp.sqrt(jnp.sum(matrix * matrix, keepdims=True))
                norm_ref[g] = jnp.broadcast_to(norm, (8, 128))
                root = matrix / norm
                keep(root_ref, g, root)
                update_of(root, g)
                vrow = vsum[0:1] + vsum[1:2]
                side = jnp.broadcast_to(vrow, (128, 128)).T
                keep(side_ref, g, side)
            for g in range(batch):
                upd = pair(upd_ref, g)
                inv_ref[g, 0] = upd[0]
                inv_ref[g, 1] = upd[1]
                keep(root_ref, g, product(pair(root_ref, g), upd))
            for step in range(1, NSI):
                for g in range(batch):
                    update_of(product(pair(inv_ref, g), pair(root_ref, g)), g)
                for g in range(batch):
                    upd = pair(upd_ref, g)
                    if step < NSI - 1:
                        inv, root = pair(inv_ref, g), pair(root_ref, g)
                        stacked = tuple(
                            jnp.concatenate([i, r], axis=0) for i, r in zip(inv, root)
                        )
                        both = product(stacked, upd)
                        keep(inv_ref, g, both[:128])
                        keep(root_ref, g, both[128:])
                    else:
                        inv = product(pair(inv_ref, g), upd)
                        keep(inv_ref, g, inv)
                        weight_ref[b * batch + g] = inv
            for g in range(batch):
                keep(side_ref, g, product(pair(inv_ref, g), pair(side_ref, g)))
            for g in range(batch):
                line = b * batch + g
                norm = norm_ref[g][0:1]
                wbar = product(pair(inv_ref, g), pair(side_ref, g)) / norm
                scale = jnp.sqrt(F32(127.0)) / jnp.sqrt(norm)
                weight_ref[line] = scale * weight_ref[line] + wbar

        fetch.wait()
        empty = jnp.zeros((128, 128), BF16)

        @pl.loop(0, gx)
        def _(r):
            for p in range(gy // 2):
                blends = []
                for c in (2 * p, 2 * p + 1):
                    at = (r + 1) * ring_y + (c + 1)
                    blend = (
                        4.0 * weight_ref[at]
                        + weight_ref[at + ring_y]
                        + weight_ref[at - ring_y]
                        + weight_ref[at + 1]
                        + weight_ref[at - 1]
                    ) * 0.125
                    blends.append(blend.astype(BF16))
                rhs = jnp.concatenate(
                    [
                        jnp.concatenate([blends[0], empty], axis=1),
                        jnp.concatenate([empty, blends[1]], axis=1),
                    ],
                    axis=0,
                )
                mean = mean_ref[r].T
                lhs = jnp.concatenate([held_ref[r, 2 * p], held_ref[r, 2 * p + 1]], axis=1)
                both = jnp.dot(lhs, rhs, preferred_element_type=F32)
                for side in range(2):
                    c = 2 * p + side
                    value = both[:, 128 * side : 128 * side + 128] + mean[:, c : c + 1]
                    stage_ref[r, c] = value.astype(BF16)
            pltpu.make_async_copy(stage_ref.at[r], out_ref.at[r], out_sem.at[r]).start()

        @pl.loop(0, gx)
        def _(r):
            pltpu.make_async_copy(stage_ref.at[r], out_ref.at[r], out_sem.at[r]).wait()

    return kernel


def analyse(target, factor, shift, pieces, mean, members):
    gx, gy, cl, width = members.shape
    listed = target.shape[1]
    outer = (gx + 2 * WIDE) * (gy + 2 * WIDE)
    ring_count = (gx + 2) * (gy + 2)
    batch = BATCH_ROWS * (gy + 2)
    vmem = pl.BlockSpec(memory_space=pltpu.VMEM)
    smem = pl.BlockSpec(memory_space=pltpu.SMEM)
    hbm = pl.BlockSpec(memory_space=pl.ANY)
    halves = pltpu.VMEM((batch, 2, width, width), BF16)
    return pl.pallas_call(
        make_kernel(gx, gy, cl, listed),
        name="analyse",
        out_shape=jax.ShapeDtypeStruct(members.shape, BF16),
        in_specs=[smem] * 3 + [vmem] * 8 + [hbm],
        out_specs=hbm,
        scratch_shapes=[
            pltpu.VMEM((outer, width, width), F32),
            pltpu.VMEM((outer, 8, width), F32),
            pltpu.VMEM((ring_count, width, width), F32),
            halves, halves, halves, halves,
            pltpu.VMEM((batch, 8, width), F32),
            pltpu.VMEM(members.shape, BF16),
            pltpu.VMEM(members.shape, BF16),
            pltpu.SemaphoreType.DMA,
            pltpu.SemaphoreType.DMA((gx,)),
        ],
        compiler_params=pltpu.CompilerParams(vmem_limit_bytes=44 * 2**20),
    )(target, factor, shift, *pieces, mean, members)


def pack(obs_pert, obs_weight, innovation, neighbours, loc_weight):
    gx, gy, slot_count, width = obs_pert.shape
    listed = neighbours.shape[-1]
    first = lax.reduce_precision(loc_weight, 8, 7)
    rest = loc_weight - first
    second = lax.reduce_precision(rest, 8, 7)
    third = rest - second
    small = jnp.stack([neighbours.astype(F32), first, second, third], axis=2)
    small = jnp.pad(small, ((0, 0), (0, 0), (0, 0), (0, width - listed)))
    extra = jnp.concatenate(
        [
            obs_weight[:, :, None, :].astype(BF16),
            innovation[:, :, None, :],
            small.astype(BF16),
            jnp.zeros((gx, gy, ROWS - slot_count - 6, width), BF16),
        ],
        axis=2,
    )
    return jnp.concatenate([obs_pert, extra], axis=2)


def lists(pieces, gx, gy, listed):
    own, low, high, left, right, cleft, cright = (p[:, :, 130:134, :listed] for p in pieces)
    low, high = low[-1:], high[:1]
    left, right = left[:, -1:], right[:, :1]
    cleft = cleft[WIDE - 1 : WIDE + 1, -1:]
    cright = cright[WIDE - 1 : WIDE + 1, :1]
    middle = jnp.concatenate([left, own, right], axis=1)
    top = jnp.concatenate([cleft[:1], low, cright[:1]], axis=1)
    bottom = jnp.concatenate([cleft[1:], high, cright[1:]], axis=1)
    framed = jnp.concatenate([top, middle, bottom], axis=0).astype(F32)
    codes = framed[:, :, 0].astype(jnp.int32)
    factor = framed[:, :, 1] + framed[:, :, 2] + framed[:, :, 3]
    outer_y = gy + 2 * WIDE
    row = jnp.arange(gx + 2, dtype=jnp.int32)[:, None, None]
    col = jnp.arange(gy + 2, dtype=jnp.int32)[None, :, None]
    target = (row + codes // 5) * outer_y + col + codes % 5
    return target.reshape(-1, listed), factor.reshape(-1, listed)


def total_of(values):
    count = lax.axis_size("c")
    values = values + lax.ppermute(values, "c", ring(count, 1))
    chips = lax.axis_size("x") * lax.axis_size("y") * lax.axis_size("z")
    sent = jnp.broadcast_to(values, (chips, values.shape[1]))
    return jnp.sum(lax.all_to_all(sent, ("x", "y", "z"), 0, 0, tiled=True), axis=0)


def shards(members, mean_state, obs_pert, obs_rinv, innovation, obs_count, neighbours, loc_weight):
    gx, gy, slot_count, width = obs_pert.shape
    listed = neighbours.shape[-1]
    slots = jnp.arange(slot_count, dtype=jnp.int32)
    live_slot = slots[None, None, :] < obs_count[:, :, None]
    obs_weight = jnp.where(live_slot, obs_rinv.astype(F32), F32(0.0))
    own = pack(obs_pert, obs_weight, innovation, neighbours, loc_weight)
    tx, ty = lax.axis_size(TX), lax.axis_size(TY)
    low = lax.ppermute(own[gx - WIDE :], TX, ring(tx, 1))
    high = lax.ppermute(own[:WIDE], TX, ring(tx, -1))
    left = lax.ppermute(own[:, gy - WIDE :], TY, ring(ty, 1))
    right = lax.ppermute(own[:, :WIDE], TY, ring(ty, -1))
    cleft = lax.ppermute(
        jnp.concatenate([low[:, gy - WIDE :], high[:, gy - WIDE :]], axis=0), TY, ring(ty, 1)
    )
    cright = lax.ppermute(
        jnp.concatenate([low[:, :WIDE], high[:, :WIDE]], axis=0), TY, ring(ty, -1)
    )
    innov_f = innovation.astype(F32)
    square_sum = jnp.sum(jnp.square(obs_pert.astype(F32)), axis=-1)
    first = jnp.sum(obs_weight * innov_f * innov_f)
    second = jnp.sum(live_slot.astype(F32) + obs_weight * square_sum / (width - 1))
    lane = lax.broadcasted_iota(jnp.int32, (1, 128), 1)
    sums = total_of(jnp.where(lane == 0, first, jnp.where(lane == 1, second, 0.0)))
    shift = (width - 1) / (sums[0] / sums[1])
    pieces = (own, low, high, left, right, cleft, cright)
    target, factor = lists(pieces, gx, gy, listed)
    return analyse(target, factor, shift.reshape(1), pieces, mean_state, members)


def solution(mesh):
    finer = Mesh(mesh.devices.reshape(4, 4, 8, 2), AXES)
    return jax.shard_map(
        shards,
        mesh=finer,
        in_specs=(
            P(TX, TY, None, None),
            P(TX, TY, None),
            P(TX, TY, None, None),
            P(TX, TY, None),
            P(TX, TY, None),
            P(TX, TY),
            P(TX, TY, None),
            P(TX, TY, None),
        ),
        out_specs=P(TX, TY, None, None),
        check_vma=False,
    )
```

```python
import jax
import jax.numpy as jnp
from jax import lax
from jax.experimental import pallas as pl
from jax.experimental.pallas import tpu as pltpu
from jax.sharding import Mesh
from jax.sharding import PartitionSpec as P

F32 = jnp.float32
BF16 = jnp.bfloat16
NSI = 5
WIDE = 3
ROWS = 144
BATCH = 14
PREPARE_VMEM = 56 * 2**20
ANALYSE_VMEM = 59 * 2**20
AXES = ("x", "y", "z", "c")
TX = ("x", "y")
TY = ("z", "c")


def ring(count, shift):
    return [(i, (i + shift) % count) for i in range(count)]


def split(value):
    high = value.astype(BF16)
    return high, (value - high.astype(F32)).astype(BF16)


def product(left, right):
    lhs = jnp.concatenate(left, axis=1)
    top = jnp.concatenate(right, axis=1)
    rhs = jnp.concatenate([top, top], axis=0)
    both = jnp.dot(lhs, rhs, preferred_element_type=F32)
    half = both.shape[1] // 2
    return both[:, :half] + both[:, half:]


def block_terms(block, gram_ref, vec_ref, slot):
    pert = block[:128]
    extra = block[128:].astype(F32)
    weight, innov = extra[0:1], extra[1:2]
    scaled = (pert.astype(F32).T * weight).astype(BF16)
    high, low = split(weight * innov)
    line = lax.broadcasted_iota(jnp.int32, (16, 128), 0)
    tail = jnp.where(
        line == 0,
        jnp.broadcast_to(high.astype(F32), (16, 128)),
        jnp.where(line == 1, jnp.broadcast_to(low.astype(F32), (16, 128)), 0.0),
    ).astype(BF16)
    lhs = jnp.concatenate([scaled, tail], axis=0)
    terms = jnp.dot(lhs, pert, preferred_element_type=F32)
    gram_ref[slot] = terms[:128]
    vec_ref[slot] = terms[128:136]


def prepare_kernel(
    pert_hbm, rinv_hbm, innov_hbm, count_ref, codes_hbm, factor_hbm,
    own_ref, low_ref, high_ref, left_ref, right_ref, sums_ref,
    extra_ref, pert_ref, rinv_ref, innov_ref, codes_ref, factor_ref, sems,
):
    copies = [
        pltpu.make_async_copy(src, dst, sems.at[k])
        for k, (src, dst) in enumerate(
            [
                (rinv_hbm, rinv_ref), (innov_hbm, innov_ref), (codes_hbm, codes_ref),
                (factor_hbm, factor_ref), (pert_hbm, pert_ref),
            ]
        )
    ]
    for copy in copies:
        copy.start()
    gx, gy = own_ref.shape[:2]
    lane = lax.broadcasted_iota(jnp.int32, (1, 128), 1)
    listed = codes_ref.shape[-1]
    extra_ref[...] = jnp.zeros(extra_ref.shape, F32)
    first = jnp.zeros((1, 128), F32)
    alive = jnp.zeros((1, 128), F32)
    spread = jnp.zeros((8, 128), F32)
    for copy in copies:
        copy.wait()
    for r in range(gx):
        rinv = rinv_ref[r].astype(F32)
        innovs = innov_ref[r].astype(F32)
        codes = codes_ref[r].astype(F32)
        whole = factor_ref[r]
        one = whole.astype(BF16).astype(F32)
        two = (whole - one).astype(BF16).astype(F32)
        three = whole - one - two
        for c in range(gy):
            n = r * gy + c
            live = lane < count_ref[c, r]
            weight = jnp.where(live, rinv[c : c + 1], 0.0)
            innov = innovs[c : c + 1]
            extra_ref[n, 0:1, :] = weight
            extra_ref[n, 1:2, :] = innov
            extra_ref[n, 2:3, :listed] = codes[c : c + 1]
            extra_ref[n, 3:4, :listed] = one[c : c + 1]
            extra_ref[n, 4:5, :listed] = two[c : c + 1]
            extra_ref[n, 5:6, :listed] = three[c : c + 1]
            block = pert_ref[r, c]
            turned = block.astype(F32).T
            part = turned * turned * weight
            for k in range(16):
                spread = spread + part[8 * k : 8 * k + 8]
            first = first + weight * innov * innov
            alive = alive + jnp.where(live, 1.0, 0.0)
            places = [(own_ref, r, c)]
            if r >= gx - WIDE:
                places.append((low_ref, r - (gx - WIDE), c))
            if r < WIDE:
                places.append((high_ref, r, c))
            if c >= gy - WIDE:
                places.append((left_ref, r, c - (gy - WIDE)))
            if c < WIDE:
                places.append((right_ref, r, c))
            tile = extra_ref[n].astype(BF16)
            for ref, i, j in places:
                ref[i, j, :128] = block
                ref[i, j, 128:] = tile
    s1 = jnp.sum(first, keepdims=True)
    s2 = jnp.sum(alive, keepdims=True) + jnp.sum(spread, keepdims=True) / 127.0
    sums = jnp.where(lane == 0, s1, jnp.where(lane == 1, s2, 0.0))
    sums_ref[...] = jnp.broadcast_to(sums.reshape(1, 1, 128), sums_ref.shape)


def prepare(obs_pert, obs_rinv, innovation, obs_count, neighbours, loc_weight, devices):
    gx, gy, _, width = obs_pert.shape
    vmem = pl.BlockSpec(memory_space=pltpu.VMEM)
    hbm = pl.BlockSpec(memory_space=pltpu.HBM)
    smem = pl.BlockSpec(memory_space=pltpu.SMEM)

    def blocks(rows, cols):
        return jax.ShapeDtypeStruct((rows, cols, ROWS, width), BF16)

    return pl.pallas_call(
        prepare_kernel,
        name="prepare",
        out_shape=[
            blocks(gx, gy), blocks(WIDE, gy), blocks(WIDE, gy), blocks(gx, WIDE), blocks(gx, WIDE),
            jax.ShapeDtypeStruct((devices, 1, width), F32),
        ],
        in_specs=[hbm, hbm, hbm, smem, hbm, hbm],
        out_specs=[vmem] * 6,
        scratch_shapes=[pltpu.VMEM((gx * gy, 16, width), F32)]
        + [
            pltpu.VMEM(x.shape, x.dtype)
            for x in (obs_pert, obs_rinv, innovation, neighbours, loc_weight)
        ]
        + [pltpu.SemaphoreType.DMA((5,))],
        compiler_params=pltpu.CompilerParams(vmem_limit_bytes=PREPARE_VMEM),
    )(obs_pert, obs_rinv, innovation, obs_count.T, neighbours, loc_weight)


def gram_loop(parts, gram_ref, vec_ref):
    rows = parts[0][0].shape[0]

    @pl.loop(0, rows)
    def _(r):
        for ref, base_of in parts:
            base = base_of(r)
            for c in range(ref.shape[1]):
                block_terms(ref[r, c], gram_ref, vec_ref, base + c)


def sliced(ref, base_of, pieces):
    rows = ref.shape[0] // pieces
    return [
        (ref.at[pl.ds(k * rows, rows)], lambda r, at=k * rows: base_of(r + at))
        for k in range(pieces)
    ]


def group_lines(gx, gy):
    inner = [(r, c) for r in range(gx) for c in range(gy)]
    edge = [(-1, c) for c in range(gy)] + [(gx, c) for c in range(gy)]
    edge += [(r, -1) for r in range(gx)] + [(r, gy) for r in range(gx)]
    return [(r + 1, c + 1) for r, c in inner + edge]


def make_kernel(gx, gy, listed):
    ring_y = gy + 2
    lines = group_lines(gx, gy)
    count = len(lines)

    outer_y = gy + 2 * WIDE

    def kernel(
        place_ref, sums_hbm, mean_hbm, *refs,
    ):
        pieces_hbm, refs = refs[:7], refs[7:]
        members_ref, out_ref, refs = refs[0], refs[1], refs[2:]
        pieces, refs = refs[:7], refs[7:]
        (
            gram_ref, vec_ref, weight_ref, root_ref, inv_ref, upd_ref, norm_ref, vrow_ref,
            sums_ref, mean_ref, targets_ref, factors_ref, target_ref, factor_ref,
            held_ref, stage_ref, piece_sem, side_sem, in_sem, list_sem, out_sem,
        ) = refs
        arrivals = [
            pltpu.make_async_copy(src, dst, piece_sem.at[k])
            for k, (src, dst) in enumerate(zip(pieces_hbm, pieces))
        ]
        for copy in arrivals:
            copy.start()
        sides = [
            pltpu.make_async_copy(sums_hbm, sums_ref, side_sem.at[0]),
            pltpu.make_async_copy(mean_hbm, mean_ref, side_sem.at[1]),
        ]
        for copy in sides:
            copy.start()
        fetch = pltpu.make_async_copy(members_ref, held_ref, in_sem)
        fetch.start()
        own_ref, low_ref, high_ref, left_ref, right_ref, cleft_ref, cright_ref = pieces

        def start_of(row0, col0):
            return lambda r: (r + row0) * outer_y + col0

        def corner_of(col0):
            return lambda r: (r + jnp.where(r >= WIDE, gx, 0)) * outer_y + col0

        out = (gram_ref, vec_ref)
        arrivals[0].wait()
        gram_loop(sliced(own_ref, start_of(WIDE, WIDE), 4), *out)
        for copy in arrivals[1:]:
            copy.wait()
        for n, (i, j) in enumerate(lines):
            r, c = i - 1, j - 1
            if r < 0:
                block = low_ref[WIDE - 1, c, 128:]
            elif r >= gx:
                block = high_ref[0, c, 128:]
            elif c < 0:
                block = left_ref[r, WIDE - 1, 128:]
            elif c >= gy:
                block = right_ref[r, 0, 128:]
            else:
                block = own_ref[r, c, 128:]
            info = block.astype(F32)
            codes = info[2:3].astype(jnp.int32)
            targets_ref[n : n + 1] = (i + codes // 5) * outer_y + j + codes % 5
            factors_ref[n : n + 1] = info[3:4] + info[4:5] + info[5:6]
        copies = [
            pltpu.make_async_copy(targets_ref, target_ref, list_sem.at[0]),
            pltpu.make_async_copy(factors_ref, factor_ref, list_sem.at[1]),
        ]
        for copy in copies:
            copy.start()
        gram_loop(
            [(low_ref, start_of(0, WIDE)), (high_ref, start_of(WIDE + gx, WIDE))], *out
        )
        gram_loop(
            sliced(left_ref, start_of(WIDE, 0), 2)
            + sliced(right_ref, start_of(WIDE, WIDE + gy), 2),
            *out,
        )
        gram_loop(
            sliced(cleft_ref, corner_of(0), 2) + sliced(cright_ref, corner_of(WIDE + gy), 2), *out
        )
        for copy in sides + copies:
            copy.wait()
        sums = jnp.sum(sums_ref[...], axis=0)
        shift = 127.0 / (sums[:, 0:1] / sums[:, 1:2])
        eye = (
            lax.broadcasted_iota(jnp.int32, (128, 128), 0)
            == lax.broadcasted_iota(jnp.int32, (128, 128), 1)
        )

        def update_of(value, g):
            keep(upd_ref, g, jnp.where(eye, 1.5, 0.0) - 0.5 * value)

        def keep(ref, g, value):
            high, low = split(value)
            ref[g, 0] = high
            ref[g, 1] = low

        def pair(ref, g):
            return ref[g, 0], ref[g, 1]

        @pl.loop(0, count // BATCH)
        def _(b):
            for g in range(BATCH):
                line = b * BATCH + g
                total = jnp.zeros((128, 128), F32)
                vsum = jnp.zeros((8, 128), F32)
                for j in range(listed):
                    slot = target_ref[line, j]
                    factor = factor_ref[line, j]
                    total = total + factor * gram_ref[slot]
                    vsum = vsum + factor * vec_ref[slot]
                matrix = total + jnp.where(eye, jnp.broadcast_to(shift, (128, 128)), 0.0)
                norm = jnp.sqrt(jnp.sum(matrix * matrix, keepdims=True))
                norm_ref[g] = jnp.broadcast_to(norm, (8, 128))
                root = matrix / norm
                keep(root_ref, g, root)
                update_of(root, g)
                vrow_ref[g, 0:1] = vsum[0:1] + vsum[1:2]
            for g in range(BATCH):
                upd = pair(upd_ref, g)
                inv_ref[g, 0] = upd[0]
                inv_ref[g, 1] = upd[1]
                keep(root_ref, g, product(pair(root_ref, g), upd))
            for step in range(1, NSI):
                for g in range(BATCH):
                    update_of(product(pair(inv_ref, g), pair(root_ref, g)), g)
                for g in range(BATCH):
                    upd = pair(upd_ref, g)
                    if step < NSI - 1:
                        inv, root = pair(inv_ref, g), pair(root_ref, g)
                        stacked = tuple(
                            jnp.concatenate([i, r], axis=0) for i, r in zip(inv, root)
                        )
                        both = product(stacked, upd)
                        keep(inv_ref, g, both[:128])
                        keep(root_ref, g, both[128:])
                    else:
                        inv = product(pair(inv_ref, g), upd)
                        place = place_ref[b * BATCH + g]
                        norm = norm_ref[g][0:1]
                        once = jnp.sum(inv * vrow_ref[g, 0:1], axis=1, keepdims=True)
                        row = jnp.broadcast_to(once, (128, 128)).T[0:1]
                        wbar = jnp.sum(inv * (row / norm), axis=1, keepdims=True)
                        scale = jnp.sqrt(F32(127.0)) / jnp.sqrt(norm)
                        weight_ref[place] = scale * inv + wbar

        fetch.wait()
        empty = jnp.zeros((128, 128), BF16)

        @pl.loop(0, gx)
        def _(r):
            mean = mean_ref[r].T
            for p in range(gy // 2):
                blends = []
                for c in (2 * p, 2 * p + 1):
                    at = (r + 1) * ring_y + (c + 1)
                    blend = (
                        4.0 * weight_ref[at]
                        + weight_ref[at + ring_y]
                        + weight_ref[at - ring_y]
                        + weight_ref[at + 1]
                        + weight_ref[at - 1]
                    ) * 0.125
                    blends.append(blend.astype(BF16))
                rhs = jnp.concatenate(
                    [
                        jnp.concatenate([blends[0], empty], axis=1),
                        jnp.concatenate([empty, blends[1]], axis=1),
                    ],
                    axis=0,
                )
                lhs = jnp.concatenate([held_ref[r, 2 * p], held_ref[r, 2 * p + 1]], axis=1)
                both = jnp.dot(lhs, rhs, preferred_element_type=F32)
                for side in range(2):
                    c = 2 * p + side
                    value = both[:, 128 * side : 128 * side + 128] + mean[:, c : c + 1]
                    stage_ref[r, c] = value.astype(BF16)
            pltpu.make_async_copy(stage_ref.at[r], out_ref.at[r], out_sem.at[r]).start()

        @pl.loop(0, gx)
        def _(r):
            pltpu.make_async_copy(stage_ref.at[r], out_ref.at[r], out_sem.at[r]).wait()

    return kernel


def analyse(sums, pieces, mean, members, listed):
    gx, gy, _, width = members.shape
    outer = (gx + 2 * WIDE) * (gy + 2 * WIDE)
    lines = group_lines(gx, gy)
    place = jnp.array([i * (gy + 2) + j for i, j in lines], jnp.int32)
    smem = pl.BlockSpec(memory_space=pltpu.SMEM)
    hbm = pl.BlockSpec(memory_space=pltpu.HBM)
    halves = pltpu.VMEM((BATCH, 2, width, width), BF16)
    padded = -(-len(lines) // 8) * 8
    return pl.pallas_call(
        make_kernel(gx, gy, listed),
        name="analyse",
        out_shape=jax.ShapeDtypeStruct(members.shape, BF16),
        in_specs=[smem] + [hbm] * (3 + len(pieces)),
        out_specs=hbm,
        scratch_shapes=[pltpu.VMEM(x.shape, x.dtype) for x in pieces]
        + [
            pltpu.VMEM((outer, width, width), F32),
            pltpu.VMEM((outer, 8, width), F32),
            pltpu.VMEM(((gx + 2) * (gy + 2), width, width), F32),
            halves, halves, halves,
            pltpu.VMEM((BATCH, 8, width), F32),
            pltpu.VMEM((BATCH, 8, width), F32),
            pltpu.VMEM(sums.shape, F32),
            pltpu.VMEM(mean.shape, F32),
            pltpu.VMEM((padded, width), jnp.int32),
            pltpu.VMEM((padded, width), F32),
            pltpu.SMEM((padded, width), jnp.int32),
            pltpu.SMEM((padded, width), F32),
            pltpu.VMEM(members.shape, BF16),
            pltpu.VMEM(members.shape, BF16),
            pltpu.SemaphoreType.DMA((len(pieces),)),
            pltpu.SemaphoreType.DMA((2,)),
            pltpu.SemaphoreType.DMA,
            pltpu.SemaphoreType.DMA((2,)),
            pltpu.SemaphoreType.DMA((gx,)),
        ],
        compiler_params=pltpu.CompilerParams(vmem_limit_bytes=ANALYSE_VMEM),
    )(place, sums, mean, *pieces, members)


def shards(members, mean_state, obs_pert, obs_rinv, innovation, obs_count, neighbours, loc_weight):
    _, gy = obs_pert.shape[:2]
    tx, ty = lax.axis_size(TX), lax.axis_size(TY)
    own, last_x, first_x, last_y, first_y, sums = prepare(
        obs_pert, obs_rinv, innovation, obs_count, neighbours, loc_weight, tx * ty
    )
    low = lax.ppermute(last_x, TX, ring(tx, 1))
    high = lax.ppermute(first_x, TX, ring(tx, -1))
    sums = lax.all_to_all(sums, AXES, 0, 0, tiled=True)
    left = lax.ppermute(last_y, TY, ring(ty, 1))
    right = lax.ppermute(first_y, TY, ring(ty, -1))
    forward = jnp.concatenate([low[:, gy - WIDE :], high[:, gy - WIDE :]], axis=0)
    backward = jnp.concatenate([low[:, :WIDE], high[:, :WIDE]], axis=0)
    corners = (
        lax.ppermute(forward, TY, ring(ty, 1)),
        lax.ppermute(backward, TY, ring(ty, -1)),
    )
    listed = neighbours.shape[-1]
    pieces = (own, low, high, left, right, *corners)
    return analyse(sums, pieces, mean_state, members, listed)


def solution(mesh):
    finer = Mesh(mesh.devices.reshape(4, 4, 8, 2), AXES)
    return jax.shard_map(
        shards,
        mesh=finer,
        in_specs=(
            P(TX, TY, None, None),
            P(TX, TY, None),
            P(TX, TY, None, None),
            P(TX, TY, None),
            P(TX, TY, None),
            P(TX, TY),
            P(TX, TY, None),
            P(TX, TY, None),
        ),
        out_specs=P(TX, TY, None, None),
        check_vma=False,
    )
```

```python
import jax
import jax.numpy as jnp
from jax import lax
from jax.experimental import pallas as pl
from jax.experimental.pallas import tpu as pltpu
from jax.sharding import Mesh
from jax.sharding import PartitionSpec as P

F32 = jnp.float32
BF16 = jnp.bfloat16
NSI = 5
WIDE = 3
ROWS = 144
BATCH = 14
PREPARE_VMEM = 56 * 2**20
ANALYSE_VMEM = 59 * 2**20
AXES = ("x", "y", "z", "c")
TX = ("x", "y")
TY = ("z", "c")


def ring(count, shift):
    return [(i, (i + shift) % count) for i in range(count)]


def split(value):
    high = value.astype(BF16)
    return high, (value - high.astype(F32)).astype(BF16)


def product(left, right):
    lhs = jnp.concatenate(left, axis=1)
    top = jnp.concatenate(right, axis=1)
    rhs = jnp.concatenate([top, top], axis=0)
    both = jnp.dot(lhs, rhs, preferred_element_type=F32)
    half = both.shape[1] // 2
    return both[:, :half] + both[:, half:]


def block_terms(block, gram_ref, vec_ref, slot):
    pert = block[:128]
    extra = block[128:].astype(F32)
    weight, innov = extra[0:1], extra[1:2]
    scaled = (pert.astype(F32).T * weight).astype(BF16)
    high, low = split(weight * innov)
    line = lax.broadcasted_iota(jnp.int32, (16, 128), 0)
    tail = jnp.where(
        line == 0,
        jnp.broadcast_to(high.astype(F32), (16, 128)),
        jnp.where(line == 1, jnp.broadcast_to(low.astype(F32), (16, 128)), 0.0),
    ).astype(BF16)
    lhs = jnp.concatenate([scaled, tail], axis=0)
    terms = jnp.dot(lhs, pert, preferred_element_type=F32)
    gram_ref[slot] = terms[:128]
    vec_ref[slot] = terms[128:136]


def prepare_kernel(
    pert_hbm, rinv_hbm, innov_hbm, count_ref, codes_hbm, factor_hbm,
    own_ref, low_ref, high_ref, left_ref, right_ref, sums_ref,
    extra_ref, pert_ref, rinv_ref, innov_ref, codes_ref, factor_ref, sems,
):
    copies = [
        pltpu.make_async_copy(src, dst, sems.at[k])
        for k, (src, dst) in enumerate(
            [
                (rinv_hbm, rinv_ref), (innov_hbm, innov_ref), (codes_hbm, codes_ref),
                (factor_hbm, factor_ref), (pert_hbm, pert_ref),
            ]
        )
    ]
    for copy in copies:
        copy.start()
    gx, gy = own_ref.shape[:2]
    lane = lax.broadcasted_iota(jnp.int32, (1, 128), 1)
    listed = codes_ref.shape[-1]
    extra_ref[...] = jnp.zeros(extra_ref.shape, F32)
    first = jnp.zeros((1, 128), F32)
    alive = jnp.zeros((1, 128), F32)
    spread = jnp.zeros((8, 128), F32)
    for copy in copies:
        copy.wait()
    for r in range(gx):
        rinv = rinv_ref[r].astype(F32)
        innovs = innov_ref[r].astype(F32)
        codes = codes_ref[r].astype(F32)
        whole = factor_ref[r]
        one = whole.astype(BF16).astype(F32)
        two = (whole - one).astype(BF16).astype(F32)
        three = whole - one - two
        for c in range(gy):
            n = r * gy + c
            live = lane < count_ref[c, r]
            weight = jnp.where(live, rinv[c : c + 1], 0.0)
            innov = innovs[c : c + 1]
            extra_ref[n, 0:1, :] = weight
            extra_ref[n, 1:2, :] = innov
            extra_ref[n, 2:3, :listed] = codes[c : c + 1]
            extra_ref[n, 3:4, :listed] = one[c : c + 1]
            extra_ref[n, 4:5, :listed] = two[c : c + 1]
            extra_ref[n, 5:6, :listed] = three[c : c + 1]
            block = pert_ref[r, c]
            turned = block.astype(F32).T
            part = turned * turned * weight
            for k in range(16):
                spread = spread + part[8 * k : 8 * k + 8]
            first = first + weight * innov * innov
            alive = alive + jnp.where(live, 1.0, 0.0)
            places = [(own_ref, r, c)]
            if r >= gx - WIDE:
                places.append((low_ref, r - (gx - WIDE), c))
            if r < WIDE:
                places.append((high_ref, r, c))
            if c >= gy - WIDE:
                places.append((left_ref, r, c - (gy - WIDE)))
            if c < WIDE:
                places.append((right_ref, r, c))
            tile = extra_ref[n].astype(BF16)
            for ref, i, j in places:
                ref[i, j, :128] = block
                ref[i, j, 128:] = tile
    s1 = jnp.sum(first, keepdims=True)
    s2 = jnp.sum(alive, keepdims=True) + jnp.sum(spread, keepdims=True) / 127.0
    sums = jnp.where(lane == 0, s1, jnp.where(lane == 1, s2, 0.0))
    sums_ref[...] = sums


def combine(own, other, devices):
    vmem = pl.BlockSpec(memory_space=pltpu.VMEM)

    def kernel(own_ref, other_ref, out_ref):
        both = own_ref[...] + other_ref[...]
        out_ref[...] = jnp.broadcast_to(both.reshape(1, 1, 128), out_ref.shape)

    return pl.pallas_call(
        kernel,
        name="combine",
        out_shape=jax.ShapeDtypeStruct((devices, 1, own.shape[1]), F32),
        in_specs=[vmem, vmem],
        out_specs=vmem,
        compiler_params=pltpu.CompilerParams(vmem_limit_bytes=2**20),
    )(own, other)


def prepare(obs_pert, obs_rinv, innovation, obs_count, neighbours, loc_weight):
    gx, gy, _, width = obs_pert.shape
    vmem = pl.BlockSpec(memory_space=pltpu.VMEM)
    hbm = pl.BlockSpec(memory_space=pltpu.HBM)
    smem = pl.BlockSpec(memory_space=pltpu.SMEM)

    def blocks(rows, cols):
        return jax.ShapeDtypeStruct((rows, cols, ROWS, width), BF16)

    return pl.pallas_call(
        prepare_kernel,
        name="prepare",
        out_shape=[
            blocks(gx, gy), blocks(WIDE, gy), blocks(WIDE, gy), blocks(gx, WIDE), blocks(gx, WIDE),
            jax.ShapeDtypeStruct((1, width), F32),
        ],
        in_specs=[hbm, hbm, hbm, smem, hbm, hbm],
        out_specs=[vmem] * 6,
        scratch_shapes=[pltpu.VMEM((gx * gy, 16, width), F32)]
        + [
            pltpu.VMEM(x.shape, x.dtype)
            for x in (obs_pert, obs_rinv, innovation, neighbours, loc_weight)
        ]
        + [pltpu.SemaphoreType.DMA((5,))],
        compiler_params=pltpu.CompilerParams(vmem_limit_bytes=PREPARE_VMEM),
    )(obs_pert, obs_rinv, innovation, obs_count.T, neighbours, loc_weight)


def gram_loop(parts, gram_ref, vec_ref):
    rows = parts[0][0].shape[0]

    @pl.loop(0, rows)
    def _(r):
        for ref, base_of in parts:
            base = base_of(r)
            for c in range(ref.shape[1]):
                block_terms(ref[r, c], gram_ref, vec_ref, base + c)


def sliced(ref, base_of, pieces):
    rows = ref.shape[0] // pieces
    return [
        (ref.at[pl.ds(k * rows, rows)], lambda r, at=k * rows: base_of(r + at))
        for k in range(pieces)
    ]


def group_lines(gx, gy):
    inner = [(r, c) for r in range(gx) for c in range(gy)]
    edge = [(-1, c) for c in range(gy)] + [(gx, c) for c in range(gy)]
    edge += [(r, -1) for r in range(gx)] + [(r, gy) for r in range(gx)]
    return [(r + 1, c + 1) for r, c in inner + edge]


def make_kernel(gx, gy, listed):
    ring_y = gy + 2
    lines = group_lines(gx, gy)
    count = len(lines)

    outer_y = gy + 2 * WIDE

    def kernel(
        place_ref, sums_hbm, mean_hbm, *refs,
    ):
        pieces_hbm, refs = refs[:7], refs[7:]
        members_ref, out_ref, refs = refs[0], refs[1], refs[2:]
        pieces, refs = refs[:7], refs[7:]
        (
            gram_ref, vec_ref, weight_ref, root_ref, inv_ref, upd_ref, norm_ref, vrow_ref,
            sums_ref, mean_ref, targets_ref, factors_ref, target_ref, factor_ref,
            held_ref, stage_ref, piece_sem, side_sem, in_sem, list_sem, out_sem,
        ) = refs
        arrivals = [
            pltpu.make_async_copy(src, dst, piece_sem.at[k])
            for k, (src, dst) in enumerate(zip(pieces_hbm, pieces))
        ]
        for copy in arrivals:
            copy.start()
        sides = [
            pltpu.make_async_copy(sums_hbm, sums_ref, side_sem.at[0]),
            pltpu.make_async_copy(mean_hbm, mean_ref, side_sem.at[1]),
        ]
        for copy in sides:
            copy.start()
        fetch = pltpu.make_async_copy(members_ref, held_ref, in_sem)
        fetch.start()
        own_ref, low_ref, high_ref, left_ref, right_ref, cleft_ref, cright_ref = pieces

        def start_of(row0, col0):
            return lambda r: (r + row0) * outer_y + col0

        def corner_of(col0):
            return lambda r: (r + jnp.where(r >= WIDE, gx, 0)) * outer_y + col0

        out = (gram_ref, vec_ref)
        arrivals[0].wait()
        gram_loop(sliced(own_ref, start_of(WIDE, WIDE), 4), *out)
        for copy in arrivals[1:]:
            copy.wait()
        for n, (i, j) in enumerate(lines):
            r, c = i - 1, j - 1
            if r < 0:
                block = low_ref[WIDE - 1, c, 128:]
            elif r >= gx:
                block = high_ref[0, c, 128:]
            elif c < 0:
                block = left_ref[r, WIDE - 1, 128:]
            elif c >= gy:
                block = right_ref[r, 0, 128:]
            else:
                block = own_ref[r, c, 128:]
            info = block.astype(F32)
            codes = info[2:3].astype(jnp.int32)
            targets_ref[n : n + 1] = (i + codes // 5) * outer_y + j + codes % 5
            factors_ref[n : n + 1] = info[3:4] + info[4:5] + info[5:6]
        copies = [
            pltpu.make_async_copy(targets_ref, target_ref, list_sem.at[0]),
            pltpu.make_async_copy(factors_ref, factor_ref, list_sem.at[1]),
        ]
        for copy in copies:
            copy.start()
        gram_loop(
            [(low_ref, start_of(0, WIDE)), (high_ref, start_of(WIDE + gx, WIDE))], *out
        )
        gram_loop(
            sliced(left_ref, start_of(WIDE, 0), 2)
            + sliced(right_ref, start_of(WIDE, WIDE + gy), 2),
            *out,
        )
        gram_loop(
            sliced(cleft_ref, corner_of(0), 2) + sliced(cright_ref, corner_of(WIDE + gy), 2), *out
        )
        for copy in sides + copies:
            copy.wait()
        sums = jnp.sum(sums_ref[...], axis=0)
        shift = 127.0 / (sums[:, 0:1] / sums[:, 1:2])
        eye = (
            lax.broadcasted_iota(jnp.int32, (128, 128), 0)
            == lax.broadcasted_iota(jnp.int32, (128, 128), 1)
        )

        def update_of(value, g):
            keep(upd_ref, g, jnp.where(eye, 1.5, 0.0) - 0.5 * value)

        def keep(ref, g, value):
            high, low = split(value)
            ref[g, 0] = high
            ref[g, 1] = low

        def pair(ref, g):
            return ref[g, 0], ref[g, 1]

        @pl.loop(0, count // BATCH)
        def _(b):
            for g in range(BATCH):
                line = b * BATCH + g
                total = jnp.zeros((128, 128), F32)
                vsum = jnp.zeros((8, 128), F32)
                for j in range(listed):
                    slot = target_ref[line, j]
                    factor = factor_ref[line, j]
                    total = total + factor * gram_ref[slot]
                    vsum = vsum + factor * vec_ref[slot]
                matrix = total + jnp.where(eye, jnp.broadcast_to(shift, (128, 128)), 0.0)
                norm = jnp.sqrt(jnp.sum(matrix * matrix, keepdims=True))
                norm_ref[g] = jnp.broadcast_to(norm, (8, 128))
                root = matrix / norm
                keep(root_ref, g, root)
                update_of(root, g)
                vrow_ref[g, 0:1] = vsum[0:1] + vsum[1:2]
            for g in range(BATCH):
                upd = pair(upd_ref, g)
                inv_ref[g, 0] = upd[0]
                inv_ref[g, 1] = upd[1]
                keep(root_ref, g, product(pair(root_ref, g), upd))
            for step in range(1, NSI):
                for g in range(BATCH):
                    update_of(product(pair(inv_ref, g), pair(root_ref, g)), g)
                for g in range(BATCH):
                    upd = pair(upd_ref, g)
                    if step < NSI - 1:
                        inv, root = pair(inv_ref, g), pair(root_ref, g)
                        stacked = tuple(
                            jnp.concatenate([i, r], axis=0) for i, r in zip(inv, root)
                        )
                        both = product(stacked, upd)
                        keep(inv_ref, g, both[:128])
                        keep(root_ref, g, both[128:])
                    else:
                        inv = product(pair(inv_ref, g), upd)
                        place = place_ref[b * BATCH + g]
                        norm = norm_ref[g][0:1]
                        once = jnp.sum(inv * vrow_ref[g, 0:1], axis=1, keepdims=True)
                        row = jnp.broadcast_to(once, (128, 128)).T[0:1]
                        wbar = jnp.sum(inv * (row / norm), axis=1, keepdims=True)
                        scale = jnp.sqrt(F32(127.0)) / jnp.sqrt(norm)
                        weight_ref[place] = scale * inv + wbar

        fetch.wait()
        empty = jnp.zeros((128, 128), BF16)

        @pl.loop(0, gx)
        def _(r):
            mean = mean_ref[r].T
            for p in range(gy // 2):
                blends = []
                for c in (2 * p, 2 * p + 1):
                    at = (r + 1) * ring_y + (c + 1)
                    blend = (
                        4.0 * weight_ref[at]
                        + weight_ref[at + ring_y]
                        + weight_ref[at - ring_y]
                        + weight_ref[at + 1]
                        + weight_ref[at - 1]
                    ) * 0.125
                    blends.append(blend.astype(BF16))
                rhs = jnp.concatenate(
                    [
                        jnp.concatenate([blends[0], empty], axis=1),
                        jnp.concatenate([empty, blends[1]], axis=1),
                    ],
                    axis=0,
                )
                lhs = jnp.concatenate([held_ref[r, 2 * p], held_ref[r, 2 * p + 1]], axis=1)
                both = jnp.dot(lhs, rhs, preferred_element_type=F32)
                for side in range(2):
                    c = 2 * p + side
                    value = both[:, 128 * side : 128 * side + 128] + mean[:, c : c + 1]
                    stage_ref[r, c] = value.astype(BF16)
            pltpu.make_async_copy(stage_ref.at[r], out_ref.at[r], out_sem.at[r]).start()

        @pl.loop(0, gx)
        def _(r):
            pltpu.make_async_copy(stage_ref.at[r], out_ref.at[r], out_sem.at[r]).wait()

    return kernel


def analyse(sums, pieces, mean, members, listed):
    gx, gy, _, width = members.shape
    outer = (gx + 2 * WIDE) * (gy + 2 * WIDE)
    lines = group_lines(gx, gy)
    place = jnp.array([i * (gy + 2) + j for i, j in lines], jnp.int32)
    smem = pl.BlockSpec(memory_space=pltpu.SMEM)
    hbm = pl.BlockSpec(memory_space=pltpu.HBM)
    halves = pltpu.VMEM((BATCH, 2, width, width), BF16)
    padded = -(-len(lines) // 8) * 8
    return pl.pallas_call(
        make_kernel(gx, gy, listed),
        name="analyse",
        out_shape=jax.ShapeDtypeStruct(members.shape, BF16),
        in_specs=[smem] + [hbm] * (3 + len(pieces)),
        out_specs=hbm,
        scratch_shapes=[pltpu.VMEM(x.shape, x.dtype) for x in pieces]
        + [
            pltpu.VMEM((outer, width, width), F32),
            pltpu.VMEM((outer, 8, width), F32),
            pltpu.VMEM(((gx + 2) * (gy + 2), width, width), F32),
            halves, halves, halves,
            pltpu.VMEM((BATCH, 8, width), F32),
            pltpu.VMEM((BATCH, 8, width), F32),
            pltpu.VMEM(sums.shape, F32),
            pltpu.VMEM(mean.shape, F32),
            pltpu.VMEM((padded, width), jnp.int32),
            pltpu.VMEM((padded, width), F32),
            pltpu.SMEM((padded, width), jnp.int32),
            pltpu.SMEM((padded, width), F32),
            pltpu.VMEM(members.shape, BF16),
            pltpu.VMEM(members.shape, BF16),
            pltpu.SemaphoreType.DMA((len(pieces),)),
            pltpu.SemaphoreType.DMA((2,)),
            pltpu.SemaphoreType.DMA,
            pltpu.SemaphoreType.DMA((2,)),
            pltpu.SemaphoreType.DMA((gx,)),
        ],
        compiler_params=pltpu.CompilerParams(vmem_limit_bytes=ANALYSE_VMEM),
    )(place, sums, mean, *pieces, members)


def shards(members, mean_state, obs_pert, obs_rinv, innovation, obs_count, neighbours, loc_weight):
    _, gy = obs_pert.shape[:2]
    tx, ty = lax.axis_size(TX), lax.axis_size(TY)
    own, last_x, first_x, last_y, first_y, sums = prepare(
        obs_pert, obs_rinv, innovation, obs_count, neighbours, loc_weight
    )
    cores = lax.axis_size("c")
    other = lax.ppermute(sums, "c", ring(cores, 1))
    low = lax.ppermute(last_x, TX, ring(tx, 1))
    high = lax.ppermute(first_x, TX, ring(tx, -1))
    sums = combine(sums, other, tx * ty // cores)
    sums = lax.all_to_all(sums, ("x", "y", "z"), 0, 0, tiled=True)
    left = lax.ppermute(last_y, TY, ring(ty, 1))
    right = lax.ppermute(first_y, TY, ring(ty, -1))
    forward = jnp.concatenate([low[:, gy - WIDE :], high[:, gy - WIDE :]], axis=0)
    backward = jnp.concatenate([low[:, :WIDE], high[:, :WIDE]], axis=0)
    corners = (
        lax.ppermute(forward, TY, ring(ty, 1)),
        lax.ppermute(backward, TY, ring(ty, -1)),
    )
    listed = neighbours.shape[-1]
    pieces = (own, low, high, left, right, *corners)
    return analyse(sums, pieces, mean_state, members, listed)


def solution(mesh):
    finer = Mesh(mesh.devices.reshape(4, 4, 8, 2), AXES)
    return jax.shard_map(
        shards,
        mesh=finer,
        in_specs=(
            P(TX, TY, None, None),
            P(TX, TY, None),
            P(TX, TY, None, None),
            P(TX, TY, None),
            P(TX, TY, None),
            P(TX, TY),
            P(TX, TY, None),
            P(TX, TY, None),
        ),
        out_specs=P(TX, TY, None, None),
        check_vma=False,
    )
```

```python
import jax
import jax.numpy as jnp
from jax import lax
from jax.experimental import pallas as pl
from jax.experimental.pallas import tpu as pltpu
from jax.sharding import Mesh
from jax.sharding import PartitionSpec as P

F32 = jnp.float32
BF16 = jnp.bfloat16
NSI = 5
WIDE = 3
ROWS = 144
BATCH = 14
PREPARE_VMEM = 56 * 2**20
ANALYSE_VMEM = 59 * 2**20
AXES = ("x", "y", "z", "c")
TX = ("x", "y")
TY = ("z", "c")


def ring(count, shift):
    return [(i, (i + shift) % count) for i in range(count)]


def split(value):
    high = value.astype(BF16)
    return high, (value - high.astype(F32)).astype(BF16)


def product(left, right):
    lhs = jnp.concatenate(left, axis=1)
    top = jnp.concatenate(right, axis=1)
    rhs = jnp.concatenate([top, top], axis=0)
    both = jnp.dot(lhs, rhs, preferred_element_type=F32)
    half = both.shape[1] // 2
    return both[:, :half] + both[:, half:]


def block_terms(block, gram_ref, vec_ref, slot):
    pert = block[:128]
    extra = block[128:].astype(F32)
    weight, innov = extra[0:1], extra[1:2]
    scaled = (pert.astype(F32).T * weight).astype(BF16)
    high, low = split(weight * innov)
    line = lax.broadcasted_iota(jnp.int32, (16, 128), 0)
    tail = jnp.where(
        line == 0,
        jnp.broadcast_to(high.astype(F32), (16, 128)),
        jnp.where(line == 1, jnp.broadcast_to(low.astype(F32), (16, 128)), 0.0),
    ).astype(BF16)
    lhs = jnp.concatenate([scaled, tail], axis=0)
    terms = jnp.dot(lhs, pert, preferred_element_type=F32)
    gram_ref[slot] = terms[:128]
    vec_ref[slot] = terms[128:136]


def prepare_kernel(
    pert_hbm, rinv_hbm, innov_hbm, count_ref, codes_hbm, factor_hbm,
    own_ref, low_ref, high_ref, left_ref, right_ref, sums_ref,
    extra_ref, pert_ref, rinv_ref, innov_ref, codes_ref, factor_ref, sems,
):
    copies = [
        pltpu.make_async_copy(src, dst, sems.at[k])
        for k, (src, dst) in enumerate(
            [
                (rinv_hbm, rinv_ref), (innov_hbm, innov_ref), (codes_hbm, codes_ref),
                (factor_hbm, factor_ref), (pert_hbm, pert_ref),
            ]
        )
    ]
    for copy in copies:
        copy.start()
    gx, gy = own_ref.shape[:2]
    lane = lax.broadcasted_iota(jnp.int32, (1, 128), 1)
    listed = codes_ref.shape[-1]
    extra_ref[...] = jnp.zeros(extra_ref.shape, F32)
    first = jnp.zeros((1, 128), F32)
    alive = jnp.zeros((1, 128), F32)
    spread = jnp.zeros((8, 128), F32)
    for copy in copies:
        copy.wait()
    for r in range(gx):
        rinv = rinv_ref[r].astype(F32)
        innovs = innov_ref[r].astype(F32)
        codes = codes_ref[r].astype(F32)
        whole = factor_ref[r]
        one = whole.astype(BF16).astype(F32)
        two = (whole - one).astype(BF16).astype(F32)
        three = whole - one - two
        for c in range(gy):
            n = r * gy + c
            live = lane < count_ref[c, r]
            weight = jnp.where(live, rinv[c : c + 1], 0.0)
            innov = innovs[c : c + 1]
            extra_ref[n, 0:1, :] = weight
            extra_ref[n, 1:2, :] = innov
            extra_ref[n, 2:3, :listed] = codes[c : c + 1]
            extra_ref[n, 3:4, :listed] = one[c : c + 1]
            extra_ref[n, 4:5, :listed] = two[c : c + 1]
            extra_ref[n, 5:6, :listed] = three[c : c + 1]
            block = pert_ref[r, c]
            turned = block.astype(F32).T
            part = turned * turned * weight
            for k in range(16):
                spread = spread + part[8 * k : 8 * k + 8]
            first = first + weight * innov * innov
            alive = alive + jnp.where(live, 1.0, 0.0)
            places = [(own_ref, r, c)]
            if r >= gx - WIDE:
                places.append((low_ref, r - (gx - WIDE), c))
            if r < WIDE:
                places.append((high_ref, r, c))
            if c >= gy - WIDE:
                places.append((left_ref, r, c - (gy - WIDE)))
            if c < WIDE:
                places.append((right_ref, r, c))
            tile = extra_ref[n].astype(BF16)
            for ref, i, j in places:
                ref[i, j, :128] = block
                ref[i, j, 128:] = tile
    s1 = jnp.sum(first, keepdims=True)
    s2 = jnp.sum(alive, keepdims=True) + jnp.sum(spread, keepdims=True) / 127.0
    sums = jnp.where(lane == 0, s1, jnp.where(lane == 1, s2, 0.0))
    sums_ref[...] = sums


def combine(own, other, devices):
    vmem = pl.BlockSpec(memory_space=pltpu.VMEM)

    def kernel(own_ref, other_ref, out_ref):
        both = own_ref[...] + other_ref[...]
        out_ref[...] = jnp.broadcast_to(both.reshape(1, 1, 128), out_ref.shape)

    return pl.pallas_call(
        kernel,
        name="combine",
        out_shape=jax.ShapeDtypeStruct((devices, 1, own.shape[1]), F32),
        in_specs=[vmem, vmem],
        out_specs=vmem,
        compiler_params=pltpu.CompilerParams(vmem_limit_bytes=2**20),
    )(own, other)


def prepare(obs_pert, obs_rinv, innovation, obs_count, neighbours, loc_weight):
    gx, gy, _, width = obs_pert.shape
    vmem = pl.BlockSpec(memory_space=pltpu.VMEM)
    hbm = pl.BlockSpec(memory_space=pltpu.HBM)
    smem = pl.BlockSpec(memory_space=pltpu.SMEM)

    def blocks(rows, cols):
        return jax.ShapeDtypeStruct((rows, cols, ROWS, width), BF16)

    return pl.pallas_call(
        prepare_kernel,
        name="prepare",
        out_shape=[
            blocks(gx, gy), blocks(WIDE, gy), blocks(WIDE, gy), blocks(gx, WIDE), blocks(gx, WIDE),
            jax.ShapeDtypeStruct((1, width), F32),
        ],
        in_specs=[hbm, hbm, hbm, smem, hbm, hbm],
        out_specs=[vmem] * 6,
        scratch_shapes=[pltpu.VMEM((gx * gy, 16, width), F32)]
        + [
            pltpu.VMEM(x.shape, x.dtype)
            for x in (obs_pert, obs_rinv, innovation, neighbours, loc_weight)
        ]
        + [pltpu.SemaphoreType.DMA((5,))],
        compiler_params=pltpu.CompilerParams(vmem_limit_bytes=PREPARE_VMEM),
    )(obs_pert, obs_rinv, innovation, obs_count.T, neighbours, loc_weight)


def gram_loop(parts, gram_ref, vec_ref):
    rows = parts[0][0].shape[0]

    @pl.loop(0, rows)
    def _(r):
        for ref, base_of in parts:
            base = base_of(r)
            for c in range(ref.shape[1]):
                block_terms(ref[r, c], gram_ref, vec_ref, base + c)


def sliced(ref, base_of, pieces):
    rows = ref.shape[0] // pieces
    return [
        (ref.at[pl.ds(k * rows, rows)], lambda r, at=k * rows: base_of(r + at))
        for k in range(pieces)
    ]


def group_lines(gx, gy):
    inner = [(r, c) for r in range(gx) for c in range(gy)]
    edge = [(-1, c) for c in range(gy)] + [(gx, c) for c in range(gy)]
    edge += [(r, -1) for r in range(gx)] + [(r, gy) for r in range(gx)]
    return [(r + 1, c + 1) for r, c in inner + edge]


def make_kernel(gx, gy, listed):
    ring_y = gy + 2
    lines = group_lines(gx, gy)
    count = len(lines)

    outer_y = gy + 2 * WIDE

    def kernel(
        place_ref, sums_hbm, mean_hbm, *refs,
    ):
        pieces_hbm, refs = refs[:7], refs[7:]
        members_ref, out_ref, refs = refs[0], refs[1], refs[2:]
        pieces, refs = refs[:7], refs[7:]
        (
            gram_ref, vec_ref, weight_ref, root_ref, inv_ref, upd_ref, norm_ref, vrow_ref,
            next_ref, next_vrow_ref, done_ref, done_norm_ref, done_vrow_ref,
            sums_ref, mean_ref, targets_ref, factors_ref, target_ref, factor_ref,
            held_ref, stage_ref, piece_sem, side_sem, in_sem, list_sem, out_sem,
        ) = refs
        arrivals = [
            pltpu.make_async_copy(src, dst, piece_sem.at[k])
            for k, (src, dst) in enumerate(zip(pieces_hbm, pieces))
        ]
        for copy in arrivals:
            copy.start()
        sides = [
            pltpu.make_async_copy(sums_hbm, sums_ref, side_sem.at[0]),
            pltpu.make_async_copy(mean_hbm, mean_ref, side_sem.at[1]),
        ]
        for copy in sides:
            copy.start()
        fetch = pltpu.make_async_copy(members_ref, held_ref, in_sem)
        own_ref, low_ref, high_ref, left_ref, right_ref, cleft_ref, cright_ref = pieces

        def start_of(row0, col0):
            return lambda r: (r + row0) * outer_y + col0

        def corner_of(col0):
            return lambda r: (r + jnp.where(r >= WIDE, gx, 0)) * outer_y + col0

        out = (gram_ref, vec_ref)
        arrivals[0].wait()
        gram_loop(sliced(own_ref, start_of(WIDE, WIDE), 4), *out)
        for copy in arrivals[1:]:
            copy.wait()
        fetch.start()
        for n, (i, j) in enumerate(lines):
            r, c = i - 1, j - 1
            if r < 0:
                block = low_ref[WIDE - 1, c, 128:]
            elif r >= gx:
                block = high_ref[0, c, 128:]
            elif c < 0:
                block = left_ref[r, WIDE - 1, 128:]
            elif c >= gy:
                block = right_ref[r, 0, 128:]
            else:
                block = own_ref[r, c, 128:]
            info = block.astype(F32)
            codes = info[2:3].astype(jnp.int32)
            targets_ref[n : n + 1] = (i + codes // 5) * outer_y + j + codes % 5
            factors_ref[n : n + 1] = info[3:4] + info[4:5] + info[5:6]
        copies = [
            pltpu.make_async_copy(targets_ref, target_ref, list_sem.at[0]),
            pltpu.make_async_copy(factors_ref, factor_ref, list_sem.at[1]),
        ]
        for copy in copies:
            copy.start()
        gram_loop(
            [(low_ref, start_of(0, WIDE)), (high_ref, start_of(WIDE + gx, WIDE))], *out
        )
        gram_loop(
            sliced(left_ref, start_of(WIDE, 0), 2)
            + sliced(right_ref, start_of(WIDE, WIDE + gy), 2),
            *out,
        )
        gram_loop(
            sliced(cleft_ref, corner_of(0), 2) + sliced(cright_ref, corner_of(WIDE + gy), 2), *out
        )
        for copy in sides + copies:
            copy.wait()
        sums = jnp.sum(sums_ref[...], axis=0)
        shift = 127.0 / (sums[:, 0:1] / sums[:, 1:2])
        eye = (
            lax.broadcasted_iota(jnp.int32, (128, 128), 0)
            == lax.broadcasted_iota(jnp.int32, (128, 128), 1)
        )

        def update_of(value, g):
            keep(upd_ref, g, jnp.where(eye, 1.5, 0.0) - 0.5 * value)

        def keep(ref, g, value):
            high, low = split(value)
            ref[g, 0] = high
            ref[g, 1] = low

        def pair(ref, g):
            return ref[g, 0], ref[g, 1]

        batches = count // BATCH

        def gather(line, g, seed):
            vsum = jnp.broadcast_to(seed, (8, 128))
            for j in range(listed):
                vsum = vsum + factor_ref[line, j] * vec_ref[target_ref[line, j]]
            next_vrow_ref[g, 0:1] = vsum[0:1] + vsum[1:2]
            for half in range(2):
                rows = pl.ds(64 * half, 64)
                total = jnp.broadcast_to(seed, (64, 128))
                for j in range(listed):
                    total = total + factor_ref[line, j] * gram_ref[target_ref[line, j], rows, :]
                next_ref[g, rows, :] = total

        def finish(line, g):
            inv = done_ref[g]
            norm = done_norm_ref[g][0:1]
            once = jnp.sum(inv * done_vrow_ref[g, 0:1], axis=1, keepdims=True)
            row = jnp.broadcast_to(once, (128, 128)).T[0:1]
            wbar = jnp.sum(inv * (row / norm), axis=1, keepdims=True)
            scale = jnp.sqrt(F32(127.0)) / jnp.sqrt(norm)
            weight_ref[place_ref[line]] = scale * inv + wbar

        for g in range(BATCH):
            gather(g, g, jnp.zeros((1, 128), F32))

        @pl.loop(0, batches)
        def _(b):
            ahead = jnp.minimum(b + 1, batches - 1) * BATCH
            behind = jnp.maximum(b - 1, 0) * BATCH
            for g in range(BATCH):
                matrix = next_ref[g] + jnp.where(eye, jnp.broadcast_to(shift, (128, 128)), 0.0)
                norm = jnp.sqrt(jnp.sum(matrix * matrix, keepdims=True))
                norm_ref[g] = jnp.broadcast_to(norm, (8, 128))
                vrow_ref[g, 0:1] = next_vrow_ref[g, 0:1]
                root = matrix / norm
                keep(root_ref, g, root)
                update_of(root, g)
            for g in range(BATCH):
                upd = pair(upd_ref, g)
                inv_ref[g, 0] = upd[0]
                inv_ref[g, 1] = upd[1]
                keep(root_ref, g, product(pair(root_ref, g), upd))
                finish(behind + g, g)
            for step in range(1, NSI):
                for g in range(BATCH):
                    value = product(pair(inv_ref, g), pair(root_ref, g))
                    update_of(value, g)
                    if g % 4 == 1 and (step - 1) * 4 + g // 4 < BATCH:
                        seed = jnp.where(value[0:1] > 3.0e38, 1.0e-30, 0.0)
                        k = (step - 1) * 4 + g // 4
                        gather(ahead + k, k, seed)
                for g in range(BATCH):
                    upd = pair(upd_ref, g)
                    if step < NSI - 1:
                        inv, root = pair(inv_ref, g), pair(root_ref, g)
                        stacked = tuple(
                            jnp.concatenate([i, r], axis=0) for i, r in zip(inv, root)
                        )
                        both = product(stacked, upd)
                        keep(inv_ref, g, both[:128])
                        keep(root_ref, g, both[128:])
                    else:
                        done_ref[g] = product(pair(inv_ref, g), upd)
                        done_norm_ref[g] = norm_ref[g]
                        done_vrow_ref[g, 0:1] = vrow_ref[g, 0:1]

        for g in range(BATCH):
            finish((batches - 1) * BATCH + g, g)

        fetch.wait()
        empty = jnp.zeros((128, 128), BF16)

        @pl.loop(0, gx)
        def _(r):
            mean = mean_ref[r].T
            for p in range(gy // 2):
                blends = []
                for c in (2 * p, 2 * p + 1):
                    at = (r + 1) * ring_y + (c + 1)
                    blend = (
                        4.0 * weight_ref[at]
                        + weight_ref[at + ring_y]
                        + weight_ref[at - ring_y]
                        + weight_ref[at + 1]
                        + weight_ref[at - 1]
                    ) * 0.125
                    blends.append(blend.astype(BF16))
                rhs = jnp.concatenate(
                    [
                        jnp.concatenate([blends[0], empty], axis=1),
                        jnp.concatenate([empty, blends[1]], axis=1),
                    ],
                    axis=0,
                )
                lhs = jnp.concatenate([held_ref[r, 2 * p], held_ref[r, 2 * p + 1]], axis=1)
                both = jnp.dot(lhs, rhs, preferred_element_type=F32)
                for side in range(2):
                    c = 2 * p + side
                    value = both[:, 128 * side : 128 * side + 128] + mean[:, c : c + 1]
                    stage_ref[r, c] = value.astype(BF16)
            pltpu.make_async_copy(stage_ref.at[r], out_ref.at[r], out_sem.at[r]).start()

        @pl.loop(0, gx)
        def _(r):
            pltpu.make_async_copy(stage_ref.at[r], out_ref.at[r], out_sem.at[r]).wait()

    return kernel


def analyse(sums, pieces, mean, members, listed):
    gx, gy, _, width = members.shape
    outer = (gx + 2 * WIDE) * (gy + 2 * WIDE)
    lines = group_lines(gx, gy)
    place = jnp.array([i * (gy + 2) + j for i, j in lines], jnp.int32)
    smem = pl.BlockSpec(memory_space=pltpu.SMEM)
    hbm = pl.BlockSpec(memory_space=pltpu.HBM)
    halves = pltpu.VMEM((BATCH, 2, width, width), BF16)
    padded = -(-len(lines) // 8) * 8
    return pl.pallas_call(
        make_kernel(gx, gy, listed),
        name="analyse",
        out_shape=jax.ShapeDtypeStruct(members.shape, BF16),
        in_specs=[smem] + [hbm] * (3 + len(pieces)),
        out_specs=hbm,
        scratch_shapes=[pltpu.VMEM(x.shape, x.dtype) for x in pieces]
        + [
            pltpu.VMEM((outer, width, width), F32),
            pltpu.VMEM((outer, 8, width), F32),
            pltpu.VMEM(((gx + 2) * (gy + 2), width, width), F32),
            halves, halves, halves,
            pltpu.VMEM((BATCH, 8, width), F32),
            pltpu.VMEM((BATCH, 8, width), F32),
            pltpu.VMEM((BATCH, width, width), F32),
            pltpu.VMEM((BATCH, 8, width), F32),
            pltpu.VMEM((BATCH, width, width), F32),
            pltpu.VMEM((BATCH, 8, width), F32),
            pltpu.VMEM((BATCH, 8, width), F32),
            pltpu.VMEM(sums.shape, F32),
            pltpu.VMEM(mean.shape, F32),
            pltpu.VMEM((padded, width), jnp.int32),
            pltpu.VMEM((padded, width), F32),
            pltpu.SMEM((padded, width), jnp.int32),
            pltpu.SMEM((padded, width), F32),
            pltpu.VMEM(members.shape, BF16),
            pltpu.VMEM(members.shape, BF16),
            pltpu.SemaphoreType.DMA((len(pieces),)),
            pltpu.SemaphoreType.DMA((2,)),
            pltpu.SemaphoreType.DMA,
            pltpu.SemaphoreType.DMA((2,)),
            pltpu.SemaphoreType.DMA((gx,)),
        ],
        compiler_params=pltpu.CompilerParams(vmem_limit_bytes=ANALYSE_VMEM),
    )(place, sums, mean, *pieces, members)


def shards(members, mean_state, obs_pert, obs_rinv, innovation, obs_count, neighbours, loc_weight):
    _, gy = obs_pert.shape[:2]
    tx, ty = lax.axis_size(TX), lax.axis_size(TY)
    own, last_x, first_x, last_y, first_y, sums = prepare(
        obs_pert, obs_rinv, innovation, obs_count, neighbours, loc_weight
    )
    cores = lax.axis_size("c")
    other = lax.ppermute(sums, "c", ring(cores, 1))
    low = lax.ppermute(last_x, TX, ring(tx, 1))
    high = lax.ppermute(first_x, TX, ring(tx, -1))
    sums = combine(sums, other, tx * ty // cores)
    sums = lax.all_to_all(sums, ("x", "y", "z"), 0, 0, tiled=True)
    left = lax.ppermute(last_y, TY, ring(ty, 1))
    right = lax.ppermute(first_y, TY, ring(ty, -1))
    forward = jnp.concatenate([low[:, gy - WIDE :], high[:, gy - WIDE :]], axis=0)
    backward = jnp.concatenate([low[:, :WIDE], high[:, :WIDE]], axis=0)
    corners = (
        lax.ppermute(forward, TY, ring(ty, 1)),
        lax.ppermute(backward, TY, ring(ty, -1)),
    )
    listed = neighbours.shape[-1]
    pieces = (own, low, high, left, right, *corners)
    return analyse(sums, pieces, mean_state, members, listed)


def solution(mesh):
    finer = Mesh(mesh.devices.reshape(4, 4, 8, 2), AXES)
    return jax.shard_map(
        shards,
        mesh=finer,
        in_specs=(
            P(TX, TY, None, None),
            P(TX, TY, None),
            P(TX, TY, None, None),
            P(TX, TY, None),
            P(TX, TY, None),
            P(TX, TY),
            P(TX, TY, None),
            P(TX, TY, None),
        ),
        out_specs=P(TX, TY, None, None),
        check_vma=False,
    )
```
